16 devices in a mesh: dp: 2 (over y, z), tp: 8 (over x, core).
Axes of the slice: x: 4, y: 2, z: 1, core: 2. Of those that a mesh axis runs over, the one named last changes fastest.
The devices are a block of a 4x4x8 slice.
Arguments:
- x_in: bfloat16 [256, 4096], P('dp'), parts along dimension 0
- tok_pos: int32 [256], P('dp'), parts along dimension 0
- self_k: bfloat16 [256, 64, 16, 256], P('dp', None, 'tp'), parts along dimension 0
- self_v: bfloat16 [256, 64, 16, 256], P('dp', None, 'tp'), parts along dimension 0
- cross_k: bfloat16 [256, 64, 16, 256], P('dp', None, 'tp'), parts along dimension 0
- cross_v: bfloat16 [256, 64, 16, 256], P('dp', None, 'tp'), parts along dimension 0
- enc_mask: int32 [256, 64], P('dp'), parts along dimension 0
- rel_bias: float32 [32, 16], P(None, 'tp')
- w_q: bfloat16 [4096, 4096], P(None, 'tp')
- w_k: bfloat16 [4096, 4096], P(None, 'tp')
- w_v: bfloat16 [4096, 4096], P(None, 'tp')
- w_o: bfloat16 [4096, 4096], P('tp')
- cross_q: bfloat16 [4096, 4096], P(None, 'tp')
- cross_o: bfloat16 [4096, 4096], P('tp')
- w_gate: bfloat16 [4096, 16384], P(None, 'tp')
- w_up: bfloat16 [4096, 16384], P(None, 'tp')
- w_down: bfloat16 [16384, 4096], P('tp')
- norm_self: bfloat16 [4096], replicated
- norm_cross: bfloat16 [4096], replicated
- norm_mlp: bfloat16 [4096], replicated
Outputs:
- output 1: bfloat16 [256, 4096], P('dp'), parts along dimension 0
- output 2: bfloat16 [256, 64, 16, 256], P('dp', None, 'tp'), parts along dimension 0
- output 3: bfloat16 [256, 64, 16, 256], P('dp', None, 'tp'), parts along dimension 0
There are 2 independent parts. The reference program is written for one: setup_inputs(seed, part) draws one part's arguments, and reference() takes and returns one part's arrays. A program takes and returns all parts, laid end to end along the dimension named above; an argument that names none is the same for every part.
All inputs are finite; a program needn't handle non-finite values.
Results may differ from the reference program's by a relative error of at most 0.0187279.
Values are sent between devices in bfloat16 or wider.
A program may use at most 768 MiB of HBM per device.

```python
import math
import jax
import jax.numpy as jnp
from jax import lax

BATCH_ROWS = 128
T_MAX = 64
SRC_LEN = 64
D_MODEL = 4096
N_HEADS = 16
D_HEAD = 256
D_FF = 16384

INNER_DIM = N_HEADS * D_HEAD
BUCKET_EDGES = tuple(int(math.ceil(16.0 * 8.0 ** (bucket_step / 16.0))) for bucket_step in range(1, 16))
NEG_FILL = -1e30


def draw_ends(rng_key, low_end, high_end):
    key_list = jax.random.split(rng_key, 3)
    drawn_vals = jax.random.randint(key_list[0], (BATCH_ROWS,), low_end, high_end + 1)
    high_row = jax.random.randint(key_list[1], (), 0, BATCH_ROWS)
    low_row = (high_row + jax.random.randint(key_list[2], (), 1, BATCH_ROWS)) % BATCH_ROWS
    return drawn_vals.at[high_row].set(high_end).at[low_row].set(low_end).astype(jnp.int32)


def normal_bf16(rng_key, array_shape, std_dev):
    return (std_dev * jax.random.normal(rng_key, array_shape, jnp.float32)).astype(jnp.bfloat16)


def setup_inputs(seed: int = 0, part: int = 0) -> dict:
    part_keys = jax.random.split(jax.random.fold_in(jax.random.key(seed), part), 8)
    shared_keys = jax.random.split(jax.random.key(seed + 1), 16)
    cache_shape = (BATCH_ROWS, T_MAX, N_HEADS, D_HEAD)
    cross_shape = (BATCH_ROWS, SRC_LEN, N_HEADS, D_HEAD)
    src_lens = draw_ends(part_keys[2], SRC_LEN // 4, SRC_LEN)
    bias_draw = 0.7 * jax.random.normal(shared_keys[0], (32, N_HEADS), jnp.float32)
    q_scale = (D_MODEL * D_HEAD) ** -0.5
    in_scale = D_MODEL ** -0.5
    out_scale = INNER_DIM ** -0.5
    return {
        'x_in': normal_bf16(part_keys[0], (BATCH_ROWS, D_MODEL), 1.0),
        'tok_pos': draw_ends(part_keys[1], T_MAX // 8, T_MAX - 1),
        'self_k': normal_bf16(part_keys[3], cache_shape, 1.0),
        'self_v': normal_bf16(part_keys[4], cache_shape, 1.0),
        'cross_k': normal_bf16(part_keys[5], cross_shape, 1.0),
        'cross_v': normal_bf16(part_keys[6], cross_shape, 1.0),
        'enc_mask': (jnp.arange(SRC_LEN)[None, :] < src_lens[:, None]).astype(jnp.int32),
        'rel_bias': bias_draw.at[0].add(0.5 * math.log(T_MAX) - 1.0),
        'w_q': normal_bf16(shared_keys[1], (D_MODEL, INNER_DIM), q_scale),
        'w_k': normal_bf16(shared_keys[2], (D_MODEL, INNER_DIM), in_scale),
        'w_v': normal_bf16(shared_keys[3], (D_MODEL, INNER_DIM), in_scale),
        'w_o': normal_bf16(shared_keys[4], (INNER_DIM, D_MODEL), 0.4 * math.sqrt(T_MAX) * out_scale),
        'cross_q': normal_bf16(shared_keys[5], (D_MODEL, INNER_DIM), q_scale),
        'cross_o': normal_bf16(shared_keys[6], (INNER_DIM, D_MODEL), 0.5 * math.sqrt(SRC_LEN) * out_scale),
        'w_gate': normal_bf16(shared_keys[7], (D_MODEL, D_FF), in_scale),
        'w_up': normal_bf16(shared_keys[8], (D_MODEL, D_FF), in_scale),
        'w_down': normal_bf16(shared_keys[9], (D_FF, D_MODEL), 1.5 * D_FF ** -0.5),
        'norm_self': (1.0 + 0.25 * jax.random.normal(shared_keys[10], (D_MODEL,), jnp.float32)).astype(jnp.bfloat16),
        'norm_cross': (1.0 + 0.25 * jax.random.normal(shared_keys[11], (D_MODEL,), jnp.float32)).astype(jnp.bfloat16),
        'norm_mlp': (1.0 + 0.25 * jax.random.normal(shared_keys[12], (D_MODEL,), jnp.float32)).astype(jnp.bfloat16),
    }


def rms_norm(values, norm_scale):
    inv_rms = lax.rsqrt(jnp.mean(values * values, axis=-1, keepdims=True) + 1e-6)
    return (values * inv_rms * norm_scale.astype(jnp.float32)).astype(jnp.bfloat16)


def project(normed, weight):
    return jnp.dot(normed, weight, preferred_element_type=jnp.float32).astype(jnp.bfloat16)


def rel_bucket(distance):
    bucket_edges = jnp.array(BUCKET_EDGES, dtype=jnp.int32)
    far_bucket = 16 + jnp.sum((distance[..., None] >= bucket_edges).astype(jnp.int32), axis=-1)
    return jnp.where(distance < 16, distance, far_bucket)


def attend(queries, keys_all, values_all, extra):
    def one_row(operands):
        row_q, row_k, row_v, row_extra = operands
        scores = jnp.einsum('hk,thk->ht', row_q.astype(jnp.float32), row_k.astype(jnp.float32)) + row_extra
        probs_bf = jax.nn.softmax(scores, axis=-1).astype(jnp.bfloat16)
        mixed_out = jnp.einsum('ht,thk->hk', probs_bf.astype(jnp.float32), row_v.astype(jnp.float32))
        return mixed_out.astype(jnp.bfloat16)
    return lax.map(one_row, (queries, keys_all, values_all, extra))


def reference(x_in, tok_pos, self_k, self_v, cross_k, cross_v, enc_mask, rel_bias, w_q, w_k, w_v, w_o, cross_q, cross_o, w_gate, w_up, w_down, norm_self, norm_cross, norm_mlp):
    row_count = x_in.shape[0]
    head_shape = (row_count, N_HEADS, D_HEAD)
    residual = x_in.astype(jnp.float32)
    normed = rms_norm(residual, norm_self)
    queries = project(normed, w_q).reshape(head_shape)
    new_keys = project(normed, w_k).reshape(head_shape)
    new_values = project(normed, w_v).reshape(head_shape)
    key_index = jnp.arange(T_MAX)
    at_pos = (key_index[None, :] == tok_pos[:, None])[:, :, None, None]
    new_self_k = jnp.where(at_pos, new_keys[:, None], self_k)
    new_self_v = jnp.where(at_pos, new_values[:, None], self_v)
    distance = jnp.maximum(tok_pos[:, None] - key_index[None, :], 0)
    bias_rows = jnp.swapaxes(jnp.take(rel_bias, rel_bucket(distance), axis=0), 1, 2)
    causal = (key_index[None, :] <= tok_pos[:, None])[:, None, :]
    self_extra = jnp.where(causal, bias_rows, NEG_FILL)
    mixed_self = attend(queries, new_self_k, new_self_v, self_extra)
    residual = residual + jnp.dot(mixed_self.reshape(row_count, INNER_DIM), w_o, preferred_element_type=jnp.float32)
    normed = rms_norm(residual, norm_cross)
    cross_queries = project(normed, cross_q).reshape(head_shape)
    cross_extra = jnp.where(enc_mask[:, None, :] != 0, 0.0, NEG_FILL)
    mixed_cross = attend(cross_queries, cross_k, cross_v, cross_extra)
    residual = residual + jnp.dot(mixed_cross.reshape(row_count, INNER_DIM), cross_o, preferred_element_type=jnp.float32)
    normed = rms_norm(residual, norm_mlp)
    gate_pre = jnp.dot(normed, w_gate, preferred_element_type=jnp.float32)
    up_pre = jnp.dot(normed, w_up, preferred_element_type=jnp.float32)
    hidden = (jax.nn.gelu(gate_pre, approximate=True) * up_pre).astype(jnp.bfloat16)
    residual = residual + jnp.dot(hidden, w_down, preferred_element_type=jnp.float32)
    return (residual.astype(jnp.bfloat16), new_self_k, new_self_v)
```

```python
import functools
import math
import jax
import jax.numpy as jnp
from jax import lax
from jax.experimental import pallas as pl
from jax.experimental.pallas import tpu as pltpu
from jax.sharding import PartitionSpec as P

BUCKET_EDGES = tuple(int(math.ceil(16.0 * 8.0 ** (bucket_step / 16.0))) for bucket_step in range(1, 16))
NEG_FILL = -1e30
F32 = jnp.float32
BF16 = jnp.bfloat16
MESH = pl.DeviceIdType.MESH

CHUNKS = 4
POOL = 112


def lane_ids(rows):
    return lax.broadcasted_iota(jnp.int32, (rows, 256), 1)


def cache_copies(hbm, pool, base, first, count, sem, outward=False):
    for part in range(8):
        here = pool.at[pl.ds(base + first, count), pl.ds((part // 4) * 256, 256), pl.ds((part % 4) * 128, 128)]
        there = hbm.at[pl.ds(first, count), part]
        if outward:
            yield pltpu.make_async_copy(here, there, sem)
        else:
            yield pltpu.make_async_copy(there, here, sem)


def wait_slots(pool, base, count, sem):
    whole = pool.at[pl.ds(base, count)]
    pltpu.make_async_copy(whole, whole, sem).wait()


def put_columns(columns, refs):
    rows = columns.shape[0]
    for head in range(2):
        for half in range(2):
            at = (head * 2 + half) * 128
            refs[half][pl.ds(head, rows, stride=2), :] = columns[:, at:at + 128]


def scores_pass(q_refs, pool, base, first, last, w_ref):
    row_j = lax.rem(lax.broadcasted_iota(jnp.int32, (16, 128), 0), 8) // 2
    low = lax.rem(lane_ids(8) // 2, 2) == 0

    def body(slot, carry):
        for half in range(2):
            rows = pl.ds(pl.multiple_of(slot * 16 + half * 8, 8), 8)
            both = jnp.concatenate([q_refs[0][rows, :], q_refs[1][rows, :]], axis=0)
            lhs = jnp.concatenate([jnp.where(row_j == j, both, 0.0) for j in range(4)], axis=1).astype(BF16)
            keys = pool[base + slot, half * 256:half * 256 + 256, :]
            out = lax.dot_general(lhs, keys, (((1,), (1,)), ((), ())), preferred_element_type=F32)
            w_ref[rows, :] = jnp.where(low, out[:8], out[8:])
        return carry

    lax.fori_loop(first, last, body, 0, unroll=2)


def softmax_pass(w_ref, extra_ref, p_ref, rows_total):
    step = 64
    low = lax.rem(lane_ids(step) // 2, 2) == 0

    def body(index, carry):
        rows = pl.ds(pl.multiple_of(index * step, step), step)
        w = w_ref[rows, :]
        total = w + jnp.where(low, pltpu.roll(w, 254, 1), pltpu.roll(w, 2, 1)) + extra_ref[rows, :]
        e = jnp.exp(total - jnp.max(total, axis=1, keepdims=True))
        p_ref[rows, :] = e / (0.5 * jnp.sum(e, axis=1, keepdims=True))
        return carry

    lax.fori_loop(0, rows_total // step, body, 0)


def values_pass(p_ref, pool, base, first, last, o_refs):
    row_j = lax.broadcasted_iota(jnp.int32, (8, 128), 0) // 2
    low = lax.rem(lane_ids(8) // 2, 2) == 0

    def body(slot, carry):
        for half in range(2):
            rows = pl.ds(pl.multiple_of(slot * 16 + half * 8, 8), 8)
            p = p_ref[rows, :]
            lhs = jnp.concatenate([jnp.where(low, p, 0.0), jnp.where(low, 0.0, p)], axis=0).astype(BF16)
            vals = pool[base + slot, half * 256:half * 256 + 256, :]
            out = jnp.dot(lhs, vals, preferred_element_type=F32)
            for col_half in range(2):
                acc = jnp.zeros((8, 128), F32)
                for j in range(4):
                    acc = jnp.where(row_j == j, out[col_half * 8:col_half * 8 + 8, j * 128:j * 128 + 128], acc)
                o_refs[col_half][rows, :] = acc
        return carry

    lax.fori_loop(first, last, body, 0, unroll=2)


def get_mixed(o_refs, rows, head, half):
    return o_refs[half][pl.ds(head, rows, stride=2), :].astype(BF16)


def per_row(column, ref):
    rows = column.shape[0]
    for head in range(2):
        ref[pl.ds(head, rows, stride=2), :] = column


def self_kernel(x_hbm, tok_ref, tok_row, k_hbm, v_hbm, bias_ref, wq_hbm, wk_hbm, wv_hbm, norm_ref,
                mixed_ref, nk_hbm, nv_hbm,
                x_buf, h_buf, wq, wk, wv, pool, q0, q1, nk, nv, w_ref, p_ref, extra, o0, o1, pos_ref,
                x_sem, w_sem, in_sem, out_sem):
    rows = x_buf.shape[0]
    slots = rows // 8
    groups = in_sem.shape[1]
    per = slots // groups
    x_copy = pltpu.make_async_copy(x_hbm, x_buf, x_sem)
    x_copy.start()
    w_copies = [pltpu.make_async_copy(src, dst, w_sem.at[i]) for i, (src, dst) in enumerate(((wq_hbm, wq), (wk_hbm, wk), (wv_hbm, wv)))]
    for copy in w_copies:
        copy.start()
    for which, hbm in enumerate((k_hbm, v_hbm)):
        for group in range(groups):
            for copy in cache_copies(hbm, pool, which * slots, group * per, per, in_sem.at[which, group]):
                copy.start()

    tok = jnp.broadcast_to(tok_row[...].astype(F32), (rows, rows))
    per_row(tok.T, pos_ref)

    def extra_body(index, carry):
        at = pl.ds(pl.multiple_of(index * 32, 32), 32)
        lane = lane_ids(32)
        head = lax.rem(lax.broadcasted_iota(jnp.int32, (32, 256), 0), 2)
        pos = pos_ref[at, :]
        n = jnp.concatenate([pos, pos], axis=1) - (lane // 4).astype(F32)
        bias = jnp.where(head == 0, bias_ref[0, 0], bias_ref[0, 1])
        for bucket in range(1, 32):
            edge = bucket if bucket <= 16 else BUCKET_EDGES[bucket - 17]
            if edge > nk_hbm.shape[2] // 4 - 1:
                break
            bias = jnp.where(n >= float(edge), jnp.where(head == 0, bias_ref[bucket, 0], bias_ref[bucket, 1]), bias)
        keep = jnp.logical_and(n >= 0.0, lax.rem(lane, 2) == head)
        extra[at, :] = jnp.where(keep, bias, NEG_FILL)
        return carry

    lax.fori_loop(0, 2 * rows // 32, extra_body, 0)

    x_copy.wait()

    def norm_body(index, carry):
        at = pl.ds(pl.multiple_of(index * 16, 16), 16)
        values = x_buf[at, :].astype(F32)
        inv = lax.rsqrt(jnp.mean(values * values, axis=-1, keepdims=True) + 1e-6)
        h_buf[at, :] = (values * inv * norm_ref[...].astype(F32)).astype(BF16)
        return carry

    lax.fori_loop(0, rows // 16, norm_body, 0)

    def project(weight):
        return jnp.dot(h_buf[...], weight[...], preferred_element_type=F32).astype(BF16).astype(F32)

    w_copies[0].wait()
    put_columns(project(wq), (q0, q1))
    for copy, weight, ref in ((w_copies[1], wk, nk), (w_copies[2], wv, nv)):
        copy.wait()
        columns = project(weight)
        for head in range(2):
            for half in range(2):
                at = (head * 2 + half) * 128
                for rep in range(2):
                    ref[pl.ds(rep * 4 + half * 2 + head, rows, stride=8), :] = columns[:, at:at + 128]

    row_t = lax.broadcasted_iota(jnp.int32, (16, 128), 0) // 4

    def update(base, ref, first, last):
        def body(slot, carry):
            for half in range(2):
                for j in range(4):
                    row = slot * 8 + half * 4 + j
                    p = tok_ref[row]
                    at = pl.ds(pl.multiple_of(half * 256 + (p // 4) * 16, 16), 16)
                    old = pool[base + slot, at, j * 128:j * 128 + 128].astype(F32)
                    new = ref[pl.ds(pl.multiple_of(row * 8, 8), 8), :]
                    new = jnp.concatenate([new, new], axis=0)
                    pool[base + slot, at, j * 128:j * 128 + 128] = jnp.where(row_t == lax.rem(p, 4), new, old).astype(BF16)
            return carry

        lax.fori_loop(first, last, body, 0)

    for group in range(groups):
        first = group * per
        wait_slots(pool, first, per, in_sem.at[0, group])
        update(0, nk, first, first + per)
        for copy in cache_copies(nk_hbm, pool, 0, first, per, out_sem.at[0, group], True):
            copy.start()
        scores_pass((q0, q1), pool, 0, first, first + per, w_ref)
    softmax_pass(w_ref, extra, p_ref, 2 * rows)
    for group in range(groups):
        first = group * per
        wait_slots(pool, slots + first, per, in_sem.at[1, group])
        update(slots, nv, first, first + per)
        for copy in cache_copies(nv_hbm, pool, slots, first, per, out_sem.at[1, group], True):
            copy.start()
        values_pass(p_ref, pool, slots, first, first + per, (o0, o1))
    for head in range(2):
        for half in range(2):
            at = (head * 2 + half) * 128
            mixed_ref[:, at:at + 128] = get_mixed((o0, o1), rows, head, half)
    for which in range(2):
        for group in range(groups):
            wait_slots(pool, which * slots + group * per, per, out_sem.at[which, group])


def rest_kernel(chips, x_hbm, mixed_ref, mask_ref, k_hbm, v_hbm, wo_hbm, cq_hbm, co_hbm, wg_hbm, wu_hbm, wd_hbm,
                norm_cross, norm_mlp, out_hbm,
                pool, h_buf, part, r0, s1, r1, s2, r2, res, x_own, hidden, q0, q1, w_ref, p_ref, extra, o0, o1, len_ref, mixed2,
                x_sem, pool_sem, out_sem, rs_send, rs_recv, ag_send, ag_recv):
    rows = mask_ref.shape[0]
    slots = rows // 8
    chunks, _, width = h_buf.shape
    block = x_own.shape[0]
    half_rows = block * chips
    me = lax.axis_index("tp")
    core = lax.rem(me, 2)
    chip = me // 2
    flip1 = chip + 1 - 2 * lax.rem(chip, 2)
    flip3 = chips - 1 - chip
    near1 = flip1 + core * (flip3 - flip1)
    near2 = flip3 + core * (flip1 - flip3)
    far = lax.rem(chip + 2, chips)
    peer = me + 1 - 2 * core

    def device(chip_index):
        return {"tp": chip_index * 2 + core}

    at_wo, at_cq, at_k, at_v, at_co, at_gu = 0, 8, 16, 16 + slots, 16 + 2 * slots, 24 + 2 * slots
    at_d = at_gu + 64

    def slot_of(item):
        return lax.rem(item, POOL) if not isinstance(item, int) else item % POOL

    sem_count = [0]
    waits = {}

    def load(item, src, count):
        sem = pool_sem.at[sem_count[0]]
        sem_count[0] += 1
        base = slot_of(item)
        waits[item] = (base, count, sem)
        pltpu.make_async_copy(src, pool.at[pl.ds(base, count)], sem).start()

    def load_cache(item, hbm):
        sem = pool_sem.at[sem_count[0]]
        sem_count[0] += 1
        waits[item] = (item, slots, sem)
        for copy in cache_copies(hbm, pool, item, 0, slots, sem):
            copy.start()

    def ready(item):
        base, count, sem = waits.pop(item)
        wait_slots(pool, base, count, sem)

    x_copy = pltpu.make_async_copy(x_hbm.at[pl.ds(pl.multiple_of((core * chips + chip) * block, block), block)], x_own, x_sem)
    x_copy.start()
    for n in range(8):
        load(at_wo + n, wo_hbm.at[:, :, pl.ds(n * 512, 512)], 1)
    load(at_cq, cq_hbm, 8)

    barrier = pltpu.get_barrier_semaphore()
    for other in ({"tp": peer}, device(near1), device(near2)):
        pl.semaphore_signal(barrier, inc=1, device_id=other, device_id_type=MESH)

    lens = jnp.sum(mask_ref[...].astype(F32), axis=1, keepdims=True)
    per_row(jnp.broadcast_to(lens, (rows, 128)), len_ref)

    def extra_body(index, carry):
        at = pl.ds(pl.multiple_of(index * 32, 32), 32)
        lane = lane_ids(32)
        head = lax.rem(lax.broadcasted_iota(jnp.int32, (32, 256), 0), 2)
        length = len_ref[at, :]
        inside = (lane // 4).astype(F32) < jnp.concatenate([length, length], axis=1)
        extra[at, :] = jnp.where(jnp.logical_and(inside, lax.rem(lane, 2) == head), 0.0, NEG_FILL)
        return carry

    lax.fori_loop(0, 2 * rows // 32, extra_body, 0)
    pl.semaphore_wait(barrier, 3)

    load_cache(at_k, k_hbm)
    load_cache(at_v, v_hbm)
    for n in range(8):
        load(at_co + n, co_hbm.at[:, :, pl.ds(n * 512, 512)], 1)
    gate_up = [(at_gu + 16 * (i // 2) + 8 * (i % 2), (wg_hbm, wu_hbm)[i % 2].at[:, :, pl.ds((i // 2) * 512, 512)], 8) for i in range(8)]
    down = [(at_d + 4 * n, wd_hbm.at[:, :, pl.ds(n * 512, 512)], 4) for n in range(8)]
    later = [entry for entry in gate_up + down if entry[0] + entry[2] > POOL]
    for entry in gate_up + down:
        if entry[0] + entry[2] <= POOL:
            load(*entry)

    def load_freed(limit):
        while later and slot_of(later[0][0]) + later[0][2] <= limit:
            load(*later.pop(0))

    def remote(src, dst, sends, recvs, index, target):
        return pltpu.make_async_remote_copy(src_ref=src, dst_ref=dst, send_sem=sends.at[index], recv_sem=recvs.at[index],
                                            device_id=target, device_id_type=MESH)

    def rows_of(first):
        return pl.ds(pl.multiple_of(first, block), block)

    per_chunk = width // 512

    def all_sum(make, finish):
        pending = []
        stage0 = []
        for c in range(chunks):
            for i in range(per_chunk):
                part[c, :, i * 512:i * 512 + 512] = make(c * per_chunk + i).astype(BF16)
            copy = remote(part.at[c, pl.ds(pl.multiple_of((1 - core) * half_rows, half_rows), half_rows)], r0.at[c], rs_send, rs_recv, c, {"tp": peer})
            copy.start()
            stage0.append(copy)
        stage1 = []

        def chip_sum(c, which):
            mine = part[c, rows_of(core * half_rows + which * block), :].astype(F32)
            return mine + r0[c, rows_of(which * block), :].astype(F32)

        for c in range(chunks):
            stage0[c].wait_recv()
            s1[c, 0] = chip_sum(c, near1).astype(BF16)
            s1[c, 1] = chip_sum(c, far).astype(BF16)
            copy = remote(s1.at[c], r1.at[c], rs_send, rs_recv, chunks + c, device(near1))
            copy.start()
            stage1.append(copy)
        stage2 = []
        for c in range(chunks):
            stage1[c].wait_recv()
            s2[c] = (chip_sum(c, near2) + r1[c, 1].astype(F32)).astype(BF16)
            copy = remote(s2.at[c], r2.at[c], rs_send, rs_recv, 2 * chunks + c, device(near2))
            copy.start()
            stage2.append(copy)
        for c in range(chunks):
            stage2[c].wait_recv()
            res[c] = res[c] + (chip_sum(c, chip) + r1[c, 0].astype(F32) + r2[c].astype(F32))
        for copy in stage0 + stage1 + stage2:
            copy.wait_send()

        finish_chunk = finish()

        def rows_for(core_index, chip_index):
            return rows_of((core_index * chips + chip_index) * block)

        def send(c, chip_index, kind, target):
            where = h_buf.at[c, rows_for(core, chip_index)]
            copy = remote(where, where, ag_send, ag_recv, kind * chunks + c, target)
            copy.start()
            pending.append(copy)

        def arrived(c, kind, row_slice):
            where = h_buf.at[c, row_slice]
            remote(where, where, ag_send, ag_recv, kind * chunks + c, {"tp": peer}).wait_recv()

        for c in range(chunks):
            h_buf[c, rows_for(core, chip), :] = finish_chunk(c)
            send(c, chip, 0, device(near2))
            send(c, chip, 1, device(near1))
            send(c, chip, 3, {"tp": peer})
        for c in range(chunks):
            arrived(c, 0, rows_for(core, near2))
            send(c, near2, 2, device(near1))
            send(c, near2, 4, {"tp": peer})
        for c in range(chunks):
            arrived(c, 1, rows_for(core, near1))
            send(c, near1, 5, {"tp": peer})
        for c in range(chunks):
            arrived(c, 2, rows_for(core, far))
            send(c, far, 6, {"tp": peer})
        other = 1 - core
        for c in range(chunks):
            arrived(c, 3, rows_for(other, chip))
            arrived(c, 4, rows_for(other, near1))
            arrived(c, 5, rows_for(other, near2))
            arrived(c, 6, rows_for(other, far))
        return pending

    def done(pending):
        for copy in pending:
            copy.wait_send()

    def normed(norm_ref):
        def finish():
            square = jnp.zeros((block, 1), F32)
            for c in range(chunks):
                square = square + jnp.sum(res[c] * res[c], axis=1, keepdims=True)
            inv = lax.rsqrt(square / float(chunks * width) + 1e-6)

            def chunk(c):
                return (res[c] * inv * norm_ref[:, c * width:c * width + width].astype(F32)).astype(BF16)

            return chunk

        return finish

    def plain():
        return lambda c: res[c].astype(BF16)

    def h_part(k):
        return h_buf[k // per_chunk, :, (k % per_chunk) * 512:(k % per_chunk) * 512 + 512]

    x_copy.wait()
    for c in range(chunks):
        res[c] = x_own[:, c * width:c * width + width].astype(F32)

    def make_wo(n):
        ready(at_wo + n)
        return jnp.dot(mixed_ref[...], pool[at_wo + n], preferred_element_type=F32)

    pending = all_sum(make_wo, normed(norm_cross))
    load_freed(8)

    ready(at_cq)
    queries = jnp.dot(h_part(0), pool[at_cq], preferred_element_type=F32)
    for k in range(1, 8):
        queries = queries + jnp.dot(h_part(k), pool[at_cq + k], preferred_element_type=F32)
    put_columns(queries.astype(BF16).astype(F32), (q0, q1))
    done(pending)
    load_freed(16)
    ready(at_k)
    scores_pass((q0, q1), pool, at_k, 0, slots, w_ref)
    load_freed(16 + slots)
    softmax_pass(w_ref, extra, p_ref, 2 * rows)
    ready(at_v)
    values_pass(p_ref, pool, at_v, 0, slots, (o0, o1))
    load_freed(16 + 2 * slots)
    for head in range(2):
        for half in range(2):
            at = (head * 2 + half) * 128
            mixed2[:, at:at + 128] = get_mixed((o0, o1), rows, head, half)

    def make_co(n):
        ready(at_co + n)
        return jnp.dot(mixed2[...], pool[at_co + n], preferred_element_type=F32)

    pending = all_sum(make_co, normed(norm_mlp))

    for n in range(4):
        ready(at_gu + 16 * n)
        ready(at_gu + 16 * n + 8)

    def mlp_body(n, carry):
        def product(first):
            acc = jnp.dot(h_part(0), pool[slot_of(first)], preferred_element_type=F32)
            for k in range(1, 8):
                acc = acc + jnp.dot(h_part(k), pool[slot_of(first + k)], preferred_element_type=F32)
            return acc

        gate = product(at_gu + 16 * n)
        up = product(at_gu + 16 * n + 8)
        hidden[n] = (jax.nn.gelu(gate, approximate=True) * up).astype(BF16)
        return carry

    lax.fori_loop(0, 4, mlp_body, 0)
    done(pending)

    def make_down(n):
        ready(at_d + 4 * n)
        base = slot_of(at_d + 4 * n)
        acc = jnp.dot(hidden[0], pool[base], preferred_element_type=F32)
        for k in range(1, 4):
            acc = acc + jnp.dot(hidden[k], pool[base + k], preferred_element_type=F32)
        return acc

    pending = all_sum(make_down, plain)
    copies = [pltpu.make_async_copy(h_buf.at[c], out_hbm.at[:, pl.ds(c * width, width)], out_sem.at[c]) for c in range(chunks)]
    for copy in copies:
        copy.start()
    done(pending)
    for copy in copies:
        copy.wait()


def solution(mesh):
    chips = mesh.shape["tp"] // 2
    any_space = pl.BlockSpec(memory_space=pl.ANY)
    vmem = pl.BlockSpec(memory_space=pltpu.VMEM)
    smem = pl.BlockSpec(memory_space=pltpu.SMEM)

    def local_layer(x_in, tok_pos, self_k, self_v, cross_k, cross_v, enc_mask, rel_bias, w_q, w_k, w_v, w_o, cross_q, cross_o, w_gate, w_up, w_down, norm_self, norm_cross, norm_mlp):
        rows, t_len, heads, dim = self_k.shape
        model = x_in.shape[1]
        slots = rows // 8
        flat = heads * dim

        def packed(cache):
            return cache.reshape(rows, t_len, heads, 2, 128).transpose(0, 1, 3, 2, 4).reshape(slots, 8, t_len * 4, 128)

        def unpacked(cache):
            return cache.reshape(rows, t_len, 2, heads, 128).transpose(0, 1, 3, 2, 4).reshape(rows, t_len, heads, dim)

        cache_shape = jax.ShapeDtypeStruct((slots, 8, t_len * 4, 128), BF16)
        groups = 4
        work = [pltpu.VMEM((2 * rows, 256), F32)] * 3 + [pltpu.VMEM((2 * rows, 128), F32)] * 3
        mixed, new_k, new_v = pl.pallas_call(
            self_kernel,
            name="self_attention",
            out_shape=(jax.ShapeDtypeStruct((rows, flat), BF16), cache_shape, cache_shape),
            in_specs=[any_space, smem, vmem, any_space, any_space, smem, any_space, any_space, any_space, vmem],
            out_specs=(vmem, any_space, any_space),
            scratch_shapes=[
                pltpu.VMEM((rows, model), BF16), pltpu.VMEM((rows, model), BF16),
                pltpu.VMEM((model, flat), BF16), pltpu.VMEM((model, flat), BF16), pltpu.VMEM((model, flat), BF16),
                pltpu.VMEM((2 * slots, 512, 512), BF16),
                pltpu.VMEM((2 * rows, 128), F32), pltpu.VMEM((2 * rows, 128), F32),
                pltpu.VMEM((8 * rows, 128), F32), pltpu.VMEM((8 * rows, 128), F32),
                *work,
                pltpu.SemaphoreType.DMA, pltpu.SemaphoreType.DMA((3,)),
                pltpu.SemaphoreType.DMA((2, groups)), pltpu.SemaphoreType.DMA((2, groups)),
            ],
            compiler_params=pltpu.CompilerParams(vmem_limit_bytes=63 << 20),
        )(x_in, tok_pos, tok_pos.reshape(1, rows), packed(self_k), packed(self_v), rel_bias, w_q, w_k, w_v, norm_self.reshape(1, model))

        width = model // CHUNKS
        block = rows // (2 * chips)
        x_out = pl.pallas_call(
            functools.partial(rest_kernel, chips),
            name="rest_of_layer",
            out_shape=jax.ShapeDtypeStruct((rows, model), BF16),
            in_specs=[any_space, vmem, vmem] + [any_space] * 8 + [vmem, vmem],
            out_specs=any_space,
            scratch_shapes=[
                pltpu.VMEM((POOL, 512, 512), BF16),
                pltpu.VMEM((CHUNKS, rows, width), BF16), pltpu.VMEM((CHUNKS, rows, width), BF16),
                pltpu.VMEM((CHUNKS, rows // 2, width), BF16),
                pltpu.VMEM((CHUNKS, 2, block, width), BF16), pltpu.VMEM((CHUNKS, 2, block, width), BF16),
                pltpu.VMEM((CHUNKS, block, width), BF16), pltpu.VMEM((CHUNKS, block, width), BF16),
                pltpu.VMEM((CHUNKS, block, width), F32), pltpu.VMEM((block, model), BF16),
                pltpu.VMEM((4, rows, 512), BF16),
                pltpu.VMEM((2 * rows, 128), F32), pltpu.VMEM((2 * rows, 128), F32),
                *work,
                pltpu.VMEM((rows, flat), BF16),
                pltpu.SemaphoreType.DMA, pltpu.SemaphoreType.DMA((40,)), pltpu.SemaphoreType.DMA((CHUNKS,)),
                pltpu.SemaphoreType.DMA((3 * CHUNKS,)), pltpu.SemaphoreType.DMA((3 * CHUNKS,)),
                pltpu.SemaphoreType.DMA((7 * CHUNKS,)), pltpu.SemaphoreType.DMA((7 * CHUNKS,)),
            ],
            compiler_params=pltpu.CompilerParams(collective_id=0, has_side_effects=True, vmem_limit_bytes=67_043_328),
        )(x_in, mixed, enc_mask, packed(cross_k), packed(cross_v), w_o.reshape(1, flat, model), cross_q.reshape(8, model // 8, flat),
          cross_o.reshape(1, flat, model), w_gate.reshape(8, model // 8, -1), w_up.reshape(8, model // 8, -1), w_down.reshape(4, -1, model),
          norm_cross.reshape(1, model), norm_mlp.reshape(1, model))
        return x_out, unpacked(new_k), unpacked(new_v)

    cache_spec = P('dp', None, 'tp', None)
    split_cols = P(None, 'tp')
    split_rows = P('tp', None)
    in_specs = (P('dp', None), P('dp'), cache_spec, cache_spec, cache_spec, cache_spec, P('dp', None), split_cols, split_cols, split_cols, split_cols, split_rows, split_cols, split_rows, split_cols, split_cols, split_rows, P(None), P(None), P(None))
    out_specs = (P('dp', None), cache_spec, cache_spec)
    return jax.shard_map(local_layer, mesh=mesh, in_specs=in_specs, out_specs=out_specs, check_vma=False)
```
